32 devices in a mesh: gx: 4 (over x, core), gy: 8 (over z, y).
Axes of the slice: x: 2, y: 2, z: 4, core: 2. Of those that a mesh axis runs over, the one named last changes fastest.
Arguments:
- activations: bfloat16 [4096, 8192], P('gx', 'gy'), may hold values from -12 to 12
- out_grads: bfloat16 [4096, 4096], P('gx', 'gy'), may hold values from -12 to 12
- left_roots: float32 [32, 1024, 1024], P(('gx', 'gy')), may hold values from -20 to 20, as said below
- right_roots: float32 [32, 1024, 1024], P(('gx', 'gy')), may hold values from -20 to 20, as said below
Outputs:
- update: bfloat16 [8192, 4096], P(None, 'gy')
The draws below stay inside these ranges and needn't reach their ends.
Inputs may be any that keep to these rules, and one draw needn't show every extreme that they name: `left_roots`: each block is symmetric positive definite. `right_roots`: each block is symmetric positive definite.
All inputs are finite; a program needn't handle non-finite values.
Results may differ from the reference program's by a relative error of at most 0.001.
Values may be sent and summed in bfloat16 or wider, within the bound.
A program may use at most 128 MiB of HBM per device.

```python
import math
import jax
import jax.numpy as jnp
from jax import lax

D = 8192
BLK = 1024
TOKENS = 4096
COLS = 4096
NBLK = 32
N_GY = 8


def scaled_draw(key, row_count, width):
    key_scale, key_noise = jax.random.split(key, 2)
    feature_scale = jnp.exp(jax.random.uniform(key_scale, (width,), jnp.float32, math.log(0.3), math.log(3.0)))
    values = jax.random.normal(key_noise, (row_count, width), jnp.float32) * feature_scale[None, :]
    return jnp.clip(values, -12.0, 12.0).astype(jnp.bfloat16)


def draw_activations(key, part):
    return scaled_draw(jax.random.fold_in(key, 11), TOKENS, D)


def draw_out_grads(key, part):
    return scaled_draw(jax.random.fold_in(key, 23), TOKENS, COLS)


def root_draw(key, salt):
    base = jax.random.fold_in(key, salt)

    def single(index):
        sub = jax.random.fold_in(base, index)
        key_scale, key_noise = jax.random.split(sub)
        scales = jnp.exp(jax.random.uniform(key_scale, (BLK,), jnp.float32, math.log(0.3), math.log(3.0)))
        noise = jax.random.normal(key_noise, (BLK, BLK), jnp.float32)
        symmetric = (noise + noise.T) * (0.4 / math.sqrt(2.0 * BLK))
        core = jnp.eye(BLK, dtype=jnp.float32) + symmetric
        return scales[:, None] * core * scales[None, :]
    return lax.map(single, jnp.arange(NBLK, dtype=jnp.int32))


def draw_left_roots(key, part):
    return root_draw(key, 37)


def draw_right_roots(key, part):
    return root_draw(key, 41)


def setup_inputs(seed: int = 0) -> dict:
    splits = jax.random.split(jax.random.key(seed), 5)
    activations = draw_activations(jax.random.fold_in(splits[4], 71), 0)
    out_grads = draw_out_grads(jax.random.fold_in(splits[4], 71), 0)
    left_roots = draw_left_roots(jax.random.fold_in(splits[4], 71), 0)
    right_roots = draw_right_roots(jax.random.fold_in(splits[4], 71), 0)
    return dict(activations=activations, out_grads=out_grads, left_roots=left_roots, right_roots=right_roots)


epsilon = 1e-06

def precondition(items):
    grad_block, left_root, right_root = items
    shaped = jnp.dot(jnp.dot(left_root, grad_block, precision=lax.Precision.HIGHEST), right_root, precision=lax.Precision.HIGHEST)
    graft = jnp.sqrt(jnp.mean(grad_block * grad_block) + epsilon) / jnp.sqrt(jnp.mean(shaped * shaped) + epsilon)
    return (shaped * graft).astype(jnp.bfloat16)

def reference(activations, out_grads, left_roots, right_roots):
    weight_grad = lax.dot_general(activations, out_grads, (((0,), (0,)), ((), ())), preferred_element_type=jnp.float32)
    row_blocks = D // BLK
    col_blocks = COLS // BLK
    tiles = weight_grad.reshape(row_blocks, BLK, col_blocks, BLK).transpose(0, 2, 1, 3)
    number = jnp.arange(NBLK, dtype=jnp.int32)
    row_of = (2 * (number // N_GY) + number % 2).astype(jnp.int32)
    col_of = (number % N_GY // 2).astype(jnp.int32)
    grad_blocks = tiles[row_of, col_of]
    updates = lax.map(precondition, (grad_blocks, left_roots, right_roots))
    grid_rows = jnp.arange(row_blocks, dtype=jnp.int32)[:, None]
    grid_cols = jnp.arange(col_blocks, dtype=jnp.int32)[None, :]
    owner = (grid_rows // 2 * N_GY + 2 * grid_cols + grid_rows % 2).astype(jnp.int32)
    placed = updates[owner]
    return placed.transpose(0, 2, 1, 3).reshape(D, COLS)
```

```python
import functools

import jax
import jax.numpy as jnp
from jax import lax
from jax.experimental import pallas as pl
from jax.experimental.pallas import tpu as pltpu
from jax.sharding import PartitionSpec as P

epsilon = 1e-06
MESH = pl.DeviceIdType.MESH
f32, bf16 = jnp.float32, jnp.bfloat16
COLUMN, ROW = (((0,), (0,)), ((), ())), (((1,), (0,)), ((), ()))


def dot(a, b, dims=ROW):
    return lax.dot_general(a, b, dims, preferred_element_type=f32)


def split(v):
    high = v.astype(bf16)
    return high, (v - high.astype(f32)).astype(bf16)


def kernel(
    planes, parts, a, o, left, right, out,
    af, tr, oall, stage_l, stage_r, lh, ll, rh, rl, grad, half, shaped, fin, sq_g, sq_s,
    load_sem, own_sem, src_sem, fwd_sem, tr_sem, cross_sem, af_recv, tr_recv,
    o_own, o_send, o_recv, out_own, out_send, out_recv,
):
    i, j = lax.axis_index("gx"), lax.axis_index("gy")
    x, c, z, y = i // 2, i % 2, j // 2, j % 2
    block = left.shape[1]
    width = block // parts
    half_width = block // 2
    last = planes - 1

    def dev(xx, cc, zz, yy):
        return (2 * xx + cc, 2 * zz + yy)

    def remote(src, dst, send, recv, to):
        return pltpu.make_async_remote_copy(
            src_ref=src, dst_ref=dst, send_sem=send, recv_sem=recv, device_id=to, device_id_type=MESH
        )

    loads = [
        pltpu.make_async_copy(left.at[0], stage_l, load_sem.at[0]),
        pltpu.make_async_copy(right.at[0], stage_r, load_sem.at[1]),
    ]

    def o_slot(xx, cc, yy):
        columns = pl.ds(pl.multiple_of(yy * half_width, half_width), half_width)
        return oall.at[2 * xx + cc, :, columns]

    def o_copy(src, slot, number, to):
        xx, cc, yy = slot
        return remote(src, o_slot(*slot), o_send.at[number], o_recv.at[4 * xx + 2 * cc + yy], to)

    own, over_x, over_y, over_xy = (x, c, y), (1 - x, c, y), (x, c, 1 - y), (1 - x, c, 1 - y)
    to_x, to_y, to_core = dev(1 - x, c, z, y), dev(x, c, z, 1 - y), dev(x, 1 - c, z, y)
    o_local = pltpu.make_async_copy(o, o_slot(*own), o_own)
    o_own_copies = [o_copy(o, own, 0, to_x), o_copy(o, own, 1, to_y), o_copy(o, own, 2, to_core)]
    o_relays = [
        o_copy(o_slot(*over_x), over_x, 3, to_y),
        o_copy(o_slot(*over_x), over_x, 4, to_core),
        o_copy(o_slot(*over_y), over_y, 5, to_core),
        o_copy(o_slot(*over_xy), over_xy, 6, to_core),
    ]

    def o_wait(slot):
        o_copy(o_slot(*slot), slot, 0, to_x).wait_recv()

    for copy in o_own_copies:
        copy.start()
    o_local.start()

    fx, fc = z // 2, z % 2
    is_home = jnp.logical_and(x == fx, c == fc)
    keeps = x == fx

    def source(q):
        return a.at[:, q * width : (q + 1) * width]

    def home_local(q):
        return pltpu.make_async_copy(source(q), af.at[i, q], own_sem.at[q])

    def home_remote(q):
        return remote(source(q), af.at[i, q], src_sem.at[0, q], af_recv.at[i, q], dev(fx, fc, z, y))

    def spread(q, step, kept):
        number = 1 if step > 0 else 2
        to = dev(x, fc, z + step, y)
        if kept:
            return remote(source(q), af.at[i, q], src_sem.at[number, q], af_recv.at[i, q], to)
        return remote(source(q), tr.at[c, q], src_sem.at[number, q], tr_recv.at[c, q], to)

    for q in range(parts):
        for step, inside in ((1, z < last), (-1, z > 0)):

            @pl.when(jnp.logical_and(inside, keeps))
            def _():
                spread(q, step, True).start()

            @pl.when(jnp.logical_and(inside, jnp.logical_not(keeps)))
            def _():
                spread(q, step, False).start()

        @pl.when(is_home)
        def _():
            home_local(q).start()

        @pl.when(jnp.logical_not(is_home))
        def _():
            home_remote(q).start()

    for load in loads:
        load.start()

    zf, zt = i, 2 * (1 - x) + c
    end = jnp.logical_or(z == 0, z == last)
    mid = jnp.logical_not(end)

    def away(origin):
        step = jnp.where(z > origin, 1, -1)
        goes = jnp.logical_and(z != origin, mid)
        return step, goes

    step_f, goes_f = away(zf)
    step_t, goes_t = away(zt)

    def af_forward(cc, q):
        slot = 2 * x + cc
        return remote(
            af.at[slot, q], af.at[slot, q], fwd_sem.at[cc, q], af_recv.at[slot, q],
            dev(x, c, z + step_f, y),
        )

    def tr_forward(cc, q):
        return remote(
            tr.at[cc, q], tr.at[cc, q], tr_sem.at[cc, q], tr_recv.at[cc, q],
            dev(x, c, z + step_t, y),
        )

    def tr_cross(cc, q):
        slot = 2 * x + cc
        return remote(
            tr.at[cc, q], af.at[slot, q], cross_sem.at[cc, q], af_recv.at[slot, q],
            dev(1 - x, c, z, y),
        )

    def af_wait(slot, q):
        remote(
            af.at[slot, q], af.at[slot, q], fwd_sem.at[0, q], af_recv.at[slot, q], to_x
        ).wait_recv()

    def pass_tr(q):
        for cc in range(2):
            @pl.when(z != zt)
            def _():
                remote(
                    tr.at[cc, q], tr.at[cc, q], tr_sem.at[cc, q], tr_recv.at[cc, q], to_x
                ).wait_recv()
                tr_cross(cc, q).start()

            @pl.when(goes_t)
            def _():
                tr_forward(cc, q).start()

    def pass_af(q):
        for cc in range(2):
            @pl.when(goes_f)
            def _():
                af_wait(2 * x + cc, q)
                af_forward(cc, q).start()

    o_wait(over_x)
    o_relays[0].start()
    o_relays[1].start()

    @pl.when(mid)
    def _():
        for q in range(parts // 2):
            pass_tr(q)
            pass_af(q)

    o_wait(over_y)
    o_relays[2].start()
    o_wait(over_xy)
    o_relays[3].start()

    early = jnp.logical_and(end, jnp.abs(z - zt) > jnp.abs(z - zf))

    @pl.when(mid)
    def _():
        for q in range(parts // 2, parts):
            pass_tr(q)
            pass_af(q)

    @pl.when(jnp.logical_and(end, jnp.logical_not(early)))
    def _():
        for q in range(parts):
            pass_tr(q)

    for load in loads:
        load.wait()

    tile = width
    tiles = block // tile

    @pl.loop(0, tiles)
    def _(k):
        rows = pl.ds(pl.multiple_of(k * tile, tile), tile)
        high, low = split(stage_l[rows, :])
        lh[rows, :], ll[rows, :] = high, low
        high, low = split(stage_r[rows, :])
        rh[rows, :], rl[rows, :] = high, low
        half[rows, :] = jnp.zeros((tile, block), f32)

    sq_g[...] = jnp.zeros_like(sq_g)
    sq_s[...] = jnp.zeros_like(sq_s)

    for xx, cc, yy in ((x, 1 - c, y), (1 - x, 1 - c, y), (x, 1 - c, 1 - y), (1 - x, 1 - c, 1 - y)):
        o_wait((xx, cc, yy))
    o_local.wait()

    def wait_part(q):
        for slot in range(4):
            at_home = z == zf

            @pl.when(jnp.logical_and(at_home, slot == i))
            def _():
                home_local(q).wait()

            crossed = jnp.logical_or(slot // 2 != x, end)

            @pl.when(jnp.logical_or(
                jnp.logical_and(at_home, slot != i),
                jnp.logical_and(jnp.logical_not(at_home), crossed),
            ))
            def _():
                af_wait(slot, q)

    for q in range(parts):
        wait_part(q)
        grad[...] = dot(af[0, q], oall[0], COLUMN)

        @pl.loop(1, 4)
        def _(k):
            grad[...] += dot(af[k, q], oall[k], COLUMN)

        sq_g[...] += jnp.sum(grad[...] * grad[...], axis=0, keepdims=True)
        columns = slice(q * width, (q + 1) * width)

        @pl.loop(0, tiles)
        def _(k):
            rows = pl.ds(pl.multiple_of(k * tile, tile), tile)
            gh, gl = split(grad[...])
            lhk, llk = lh[rows, columns], ll[rows, columns]
            half[rows, :] += dot(lhk, gh) + dot(llk, gh) + dot(lhk, gl)

    @pl.when(early)
    def _():
        for q in range(parts):
            pass_tr(q)

    @pl.loop(0, tiles)
    def _(k):
        rows = pl.ds(pl.multiple_of(k * tile, tile), tile)
        th, tl = split(half[rows, :])
        value = dot(th, rh[...]) + dot(tl, rh[...]) + dot(th, rl[...])
        shaped[rows, :] = value
        sq_s[...] += jnp.sum(value * value, axis=0, keepdims=True)

    count = block * block
    mean_g = jnp.sum(sq_g[...], axis=1, keepdims=True) / count
    mean_s = jnp.sum(sq_s[...], axis=1, keepdims=True) / count
    graft = jnp.sqrt(mean_g + epsilon) / jnp.sqrt(mean_s + epsilon)

    def out_slot(slot, p):
        xx, cc, yy = slot
        start = (4 * xx + 2 * cc + yy) * block + p * tile
        return out.at[pl.ds(pl.multiple_of(start, tile), tile), :]

    def out_copy(src, slot, p, number, to):
        xx, cc, yy = slot
        return remote(
            src, out_slot(slot, p), out_send.at[number, p], out_recv.at[4 * xx + 2 * cc + yy, p], to
        )

    def out_wait(slot, p):
        out_copy(out_slot(slot, p), slot, p, 0, to_x).wait_recv()

    def fin_part(side, p):
        columns = pl.ds(pl.multiple_of(side * half_width, half_width), half_width)
        return fin.at[p * tile : (p + 1) * tile, columns]

    def out_local(p):
        return pltpu.make_async_copy(fin_part(y, p), out_slot(own, p), out_own.at[p])

    def out_first(p):
        return [
            out_copy(fin_part(1 - y, p), own, p, 0, to_y),
            out_copy(fin_part(y, p), own, p, 1, to_x),
            out_copy(fin_part(y, p), own, p, 2, to_core),
        ]

    def out_relay_y(p):
        return [
            out_copy(out_slot(over_y, p), over_y, p, 3, to_x),
            out_copy(out_slot(over_y, p), over_y, p, 4, to_core),
        ]

    def out_relay_x(p):
        return out_copy(out_slot(over_x, p), over_x, p, 5, to_core)

    def out_relay_xy(p):
        return out_copy(out_slot(over_xy, p), over_xy, p, 6, to_core)

    for p in range(tiles):
        fin[p * tile : (p + 1) * tile, :] = (
            shaped[p * tile : (p + 1) * tile, :] * graft
        ).astype(bf16)
        for copy in out_first(p):
            copy.start()
        out_local(p).start()
    for p in range(tiles):
        out_wait(over_y, p)
        for copy in out_relay_y(p):
            copy.start()
    for p in range(tiles):
        out_wait(over_x, p)
        out_relay_x(p).start()
    for p in range(tiles):
        out_wait(over_xy, p)
        out_relay_xy(p).start()
    for p in range(tiles):
        for xx, yy in ((x, y), (x, 1 - y), (1 - x, y), (1 - x, 1 - y)):
            out_wait((xx, 1 - c, yy), p)
        out_local(p).wait()
        for copy in out_first(p) + out_relay_y(p) + [out_relay_x(p), out_relay_xy(p)]:
            copy.wait_send()

    for copy in o_own_copies + o_relays:
        copy.wait_send()
    for q in range(parts):
        for step, inside in ((1, z < last), (-1, z > 0)):
            @pl.when(inside)
            def _():
                spread(q, step, True).wait_send()

        @pl.when(jnp.logical_not(is_home))
        def _():
            home_remote(q).wait_send()

        for cc in range(2):
            @pl.when(z != zt)
            def _():
                tr_cross(cc, q).wait_send()

            @pl.when(goes_t)
            def _():
                tr_forward(cc, q).wait_send()

            @pl.when(goes_f)
            def _():
                af_forward(cc, q).wait_send()


def routed(planes, activations, out_grads, left_roots, right_roots):
    block = left_roots.shape[1]
    tokens = activations.shape[0]
    parts = 4
    width = block // parts
    dma = pltpu.SemaphoreType.DMA
    return pl.pallas_call(
        functools.partial(kernel, planes, parts),
        out_shape=jax.ShapeDtypeStruct((planes * 2 * block, block // 2), bf16),
        in_specs=[pl.BlockSpec(memory_space=pl.ANY)] * 4,
        out_specs=pl.BlockSpec(memory_space=pl.ANY),
        scratch_shapes=[
            pltpu.VMEM((4, parts, tokens, width), bf16),
            pltpu.VMEM((2, parts, tokens, width), bf16),
            pltpu.VMEM((4, tokens, block), bf16),
            pltpu.VMEM((block, block), f32),
            pltpu.VMEM((block, block), f32),
            pltpu.VMEM((block, block), bf16),
            pltpu.VMEM((block, block), bf16),
            pltpu.VMEM((block, block), bf16),
            pltpu.VMEM((block, block), bf16),
            pltpu.VMEM((width, block), f32),
            pltpu.VMEM((block, block), f32),
            pltpu.VMEM((block, block), f32),
            pltpu.VMEM((block, block), bf16),
            pltpu.VMEM((1, block), f32),
            pltpu.VMEM((1, block), f32),
            dma((2,)), dma((parts,)), dma((3, parts)), dma((2, parts)), dma((2, parts)),
            dma((2, parts)), dma((4, parts)), dma((2, parts)),
            dma, dma((7,)), dma((8,)), dma((parts,)), dma((7, parts)), dma((8, parts)),
        ],
        compiler_params=pltpu.CompilerParams(
            has_side_effects=True, vmem_limit_bytes=62 * 1024 * 1024
        ),
    )(activations, out_grads, left_roots, right_roots)


def partner(block, axis, distance):
    count = lax.axis_size(axis)
    route = []
    for low in range(count):
        high = low | 1 << distance
        if high != low and high < count:
            route += [(low, high), (high, low)]
    return lax.ppermute(block, axis, route)


def local(activations, out_grads, left_roots, right_roots):
    block_size = left_roots.shape[1]
    half_width = block_size // 2
    parity = lax.axis_index("gy") % 2
    is_even = parity == 0
    gathered = lax.all_gather(activations, "gy", axis=1, tiled=True)
    summed = lax.psum_scatter(
        lax.dot_general(
            gathered, out_grads, (((0,), (0,)), ((), ())), preferred_element_type=jnp.float32
        ),
        "gx",
        scatter_dimension=0,
        tiled=True,
    )
    own_part = lax.dynamic_slice_in_dim(summed, parity * block_size, block_size, 0)
    far_part = lax.dynamic_slice_in_dim(summed, (1 - parity) * block_size, block_size, 0)
    received = partner(far_part, "gy", 0)
    left_block = jnp.where(is_even, own_part, received)
    right_block = jnp.where(is_even, received, own_part)
    grad_block = jnp.concatenate([left_block, right_block], axis=1)
    shaped = jnp.dot(
        jnp.dot(left_roots[0], grad_block, precision=lax.Precision.HIGHEST),
        right_roots[0],
        precision=lax.Precision.HIGHEST,
    )
    graft = jnp.sqrt(jnp.mean(grad_block * grad_block) + epsilon) / jnp.sqrt(
        jnp.mean(shaped * shaped) + epsilon
    )
    finished = (shaped * graft).astype(jnp.bfloat16)
    own_part = lax.dynamic_slice_in_dim(finished, parity * half_width, half_width, 1)
    far_part = lax.dynamic_slice_in_dim(finished, (1 - parity) * half_width, half_width, 1)
    received = partner(far_part, "gy", 0)
    upper_rows = jnp.where(is_even, own_part, received)
    lower_rows = jnp.where(is_even, received, own_part)
    paired = jnp.concatenate([upper_rows, lower_rows], axis=0)
    return lax.all_gather(paired, "gx", axis=0, tiled=True)


def solution(mesh):
    in_specs = (
        P("gx", "gy"),
        P("gx", "gy"),
        P(("gx", "gy"), None, None),
        P(("gx", "gy"), None, None),
    )
    out_specs = P(None, "gy")
    n_gx, n_gy = mesh.shape["gx"], mesh.shape["gy"]

    def per_device(activations, out_grads, left_roots, right_roots):
        operands = activations, out_grads, left_roots, right_roots
        block = left_roots.shape[1]
        whole_blocks = activations.shape[1] == block and out_grads.shape[1] * 2 == block
        if n_gx == 4 and n_gy == 2 * n_gx and whole_blocks:
            return routed(n_gx, *operands)
        return local(*operands)

    return jax.shard_map(per_device, mesh=mesh, in_specs=in_specs, out_specs=out_specs, check_vma=False)
```

```python
import functools

import jax
import jax.numpy as jnp
from jax import lax
from jax.experimental import pallas as pl
from jax.experimental.pallas import tpu as pltpu
from jax.sharding import PartitionSpec as P

epsilon = 1e-06
MESH = pl.DeviceIdType.MESH
f32, bf16 = jnp.float32, jnp.bfloat16
COLUMN, ROW = (((0,), (0,)), ((), ())), (((1,), (0,)), ((), ()))


def dot(a, b, dims=ROW):
    return lax.dot_general(a, b, dims, preferred_element_type=f32)


def split(v):
    high = v.astype(bf16)
    return high, (v - high.astype(f32)).astype(bf16)


def kernel(
    planes, parts, a, o, left, right, out,
    af, tr, oall, stage_l, stage_r, lh, ll, rh, rl, grad, half, shaped, fin, sq_g, sq_s,
    load_sem, own_sem, src_sem, fwd_sem, tr_sem, cross_sem, af_recv, tr_recv,
    o_own, o_send, o_recv, out_own, out_send, out_recv,
):
    i, j = lax.axis_index("gx"), lax.axis_index("gy")
    x, c, z, y = i // 2, i % 2, j // 2, j % 2
    block = left.shape[1]
    width = block // parts
    half_width = block // 2
    last = planes - 1

    def dev(xx, cc, zz, yy):
        return (2 * xx + cc, 2 * zz + yy)

    def remote(src, dst, send, recv, to):
        return pltpu.make_async_remote_copy(
            src_ref=src, dst_ref=dst, send_sem=send, recv_sem=recv, device_id=to, device_id_type=MESH
        )

    loads = [
        pltpu.make_async_copy(left.at[0], stage_l, load_sem.at[0]),
        pltpu.make_async_copy(right.at[0], stage_r, load_sem.at[1]),
    ]

    def o_slot(xx, cc, yy):
        columns = pl.ds(pl.multiple_of(yy * half_width, half_width), half_width)
        return oall.at[2 * xx + cc, :, columns]

    def o_copy(src, slot, number, to):
        xx, cc, yy = slot
        return remote(src, o_slot(*slot), o_send.at[number], o_recv.at[4 * xx + 2 * cc + yy], to)

    own, over_x, over_y, over_xy = (x, c, y), (1 - x, c, y), (x, c, 1 - y), (1 - x, c, 1 - y)
    to_x, to_y, to_core = dev(1 - x, c, z, y), dev(x, c, z, 1 - y), dev(x, 1 - c, z, y)
    o_local = pltpu.make_async_copy(o, o_slot(*own), o_own)
    o_own_copies = [o_copy(o, own, 0, to_x), o_copy(o, own, 1, to_y), o_copy(o, own, 2, to_core)]
    o_relays = [
        o_copy(o_slot(*over_x), over_x, 3, to_y),
        o_copy(o_slot(*over_x), over_x, 4, to_core),
        o_copy(o_slot(*over_y), over_y, 5, to_core),
        o_copy(o_slot(*over_xy), over_xy, 6, to_core),
    ]

    def o_wait(slot):
        o_copy(o_slot(*slot), slot, 0, to_x).wait_recv()

    for copy in o_own_copies:
        copy.start()
    o_local.start()

    fx, fc = z // 2, z % 2
    is_home = jnp.logical_and(x == fx, c == fc)
    keeps = x == fx

    def source(q):
        return a.at[:, q * width : (q + 1) * width]

    def home_local(q):
        return pltpu.make_async_copy(source(q), af.at[i, q], own_sem.at[q])

    def home_remote(q):
        return remote(source(q), af.at[i, q], src_sem.at[0, q], af_recv.at[i, q], dev(fx, fc, z, y))

    def spread(q, step, kept):
        number = 1 if step > 0 else 2
        to = dev(x, fc, z + step, y)
        if kept:
            return remote(source(q), af.at[i, q], src_sem.at[number, q], af_recv.at[i, q], to)
        return remote(source(q), tr.at[c, q], src_sem.at[number, q], tr_recv.at[c, q], to)

    for q in range(parts):
        for step, inside in ((1, z < last), (-1, z > 0)):

            @pl.when(jnp.logical_and(inside, keeps))
            def _():
                spread(q, step, True).start()

            @pl.when(jnp.logical_and(inside, jnp.logical_not(keeps)))
            def _():
                spread(q, step, False).start()

        @pl.when(is_home)
        def _():
            home_local(q).start()

    for load in loads:
        load.start()

    zf, zt = i, 2 * (1 - x) + c
    end = jnp.logical_or(z == 0, z == last)
    mid = jnp.logical_not(end)

    def away(origin):
        step = jnp.where(z > origin, 1, -1)
        goes = jnp.logical_and(z != origin, mid)
        return step, goes

    step_f, goes_f = away(zf)
    step_t, goes_t = away(zt)

    def af_forward(cc, q):
        slot = 2 * x + cc
        return remote(
            af.at[slot, q], af.at[slot, q], fwd_sem.at[cc, q], af_recv.at[slot, q],
            dev(x, c, z + step_f, y),
        )

    def tr_forward(cc, q):
        return remote(
            tr.at[cc, q], tr.at[cc, q], tr_sem.at[cc, q], tr_recv.at[cc, q],
            dev(x, c, z + step_t, y),
        )

    def tr_cross(cc, q):
        slot = 2 * x + cc
        return remote(
            tr.at[cc, q], af.at[slot, q], cross_sem.at[cc, q], af_recv.at[slot, q],
            dev(1 - x, c, z, y),
        )

    def af_wait(slot, q):
        remote(
            af.at[slot, q], af.at[slot, q], fwd_sem.at[0, q], af_recv.at[slot, q], to_x
        ).wait_recv()

    def pass_tr(q):
        for cc in range(2):
            @pl.when(z != zt)
            def _():
                remote(
                    tr.at[cc, q], tr.at[cc, q], tr_sem.at[cc, q], tr_recv.at[cc, q], to_x
                ).wait_recv()
                tr_cross(cc, q).start()

            @pl.when(goes_t)
            def _():
                tr_forward(cc, q).start()

    def pass_af(q):
        for cc in range(2):
            @pl.when(goes_f)
            def _():
                af_wait(2 * x + cc, q)
                af_forward(cc, q).start()

    o_wait(over_x)
    o_relays[0].start()
    o_relays[1].start()

    @pl.when(jnp.logical_not(is_home))
    def _():
        for q in range(parts):
            home_remote(q).start()

    @pl.when(mid)
    def _():
        for q in range(parts // 2):
            pass_tr(q)
            pass_af(q)

    o_wait(over_y)
    o_relays[2].start()
    o_wait(over_xy)
    o_relays[3].start()

    early = jnp.logical_and(end, jnp.abs(z - zt) > jnp.abs(z - zf))

    @pl.when(mid)
    def _():
        for q in range(parts // 2, parts):
            pass_tr(q)
            pass_af(q)

    @pl.when(jnp.logical_and(end, jnp.logical_not(early)))
    def _():
        for q in range(parts):
            pass_tr(q)

    for load in loads:
        load.wait()

    tile = width
    tiles = block // tile

    @pl.loop(0, tiles)
    def _(k):
        rows = pl.ds(pl.multiple_of(k * tile, tile), tile)
        high, low = split(stage_l[rows, :])
        lh[rows, :], ll[rows, :] = high, low
        high, low = split(stage_r[rows, :])
        rh[rows, :], rl[rows, :] = high, low
        half[rows, :] = jnp.zeros((tile, block), f32)

    sq_g[...] = jnp.zeros_like(sq_g)
    sq_s[...] = jnp.zeros_like(sq_s)

    for xx, cc, yy in ((x, 1 - c, y), (1 - x, 1 - c, y), (x, 1 - c, 1 - y), (1 - x, 1 - c, 1 - y)):
        o_wait((xx, cc, yy))
    o_local.wait()

    def wait_part(q):
        for slot in range(4):
            at_home = z == zf

            @pl.when(jnp.logical_and(at_home, slot == i))
            def _():
                home_local(q).wait()

            crossed = jnp.logical_or(slot // 2 != x, end)

            @pl.when(jnp.logical_or(
                jnp.logical_and(at_home, slot != i),
                jnp.logical_and(jnp.logical_not(at_home), crossed),
            ))
            def _():
                af_wait(slot, q)

    for q in range(parts):
        @pl.when(early)
        def _():
            pass_tr(q)

        wait_part(q)
        grad[...] = dot(af[0, q], oall[0], COLUMN)

        @pl.loop(1, 4)
        def _(k):
            grad[...] += dot(af[k, q], oall[k], COLUMN)

        sq_g[...] += jnp.sum(grad[...] * grad[...], axis=0, keepdims=True)
        columns = slice(q * width, (q + 1) * width)

        @pl.loop(0, tiles)
        def _(k):
            rows = pl.ds(pl.multiple_of(k * tile, tile), tile)
            gh, gl = split(grad[...])
            lhk, llk = lh[rows, columns], ll[rows, columns]
            half[rows, :] += dot(lhk, gh) + dot(llk, gh) + dot(lhk, gl)

    @pl.loop(0, tiles)
    def _(k):
        rows = pl.ds(pl.multiple_of(k * tile, tile), tile)
        th, tl = split(half[rows, :])
        value = dot(th, rh[...]) + dot(tl, rh[...]) + dot(th, rl[...])
        shaped[rows, :] = value
        sq_s[...] += jnp.sum(value * value, axis=0, keepdims=True)

    count = block * block
    mean_g = jnp.sum(sq_g[...], axis=1, keepdims=True) / count
    mean_s = jnp.sum(sq_s[...], axis=1, keepdims=True) / count
    graft = jnp.sqrt(mean_g + epsilon) / jnp.sqrt(mean_s + epsilon)

    def out_slot(slot, p):
        xx, cc, yy = slot
        start = (4 * xx + 2 * cc + yy) * block + p * tile
        return out.at[pl.ds(pl.multiple_of(start, tile), tile), :]

    def out_copy(src, slot, p, number, to):
        xx, cc, yy = slot
        return remote(
            src, out_slot(slot, p), out_send.at[number, p], out_recv.at[4 * xx + 2 * cc + yy, p], to
        )

    def out_wait(slot, p):
        out_copy(out_slot(slot, p), slot, p, 0, to_x).wait_recv()

    def fin_part(side, p):
        columns = pl.ds(pl.multiple_of(side * half_width, half_width), half_width)
        return fin.at[p * tile : (p + 1) * tile, columns]

    def out_local(p):
        return pltpu.make_async_copy(fin_part(y, p), out_slot(own, p), out_own.at[p])

    def out_first(p):
        return [
            out_copy(fin_part(1 - y, p), own, p, 0, to_y),
            out_copy(fin_part(y, p), own, p, 1, to_x),
            out_copy(fin_part(y, p), own, p, 2, to_core),
        ]

    def out_relay_y(p):
        return [
            out_copy(out_slot(over_y, p), over_y, p, 3, to_x),
            out_copy(out_slot(over_y, p), over_y, p, 4, to_core),
        ]

    def out_relay_x(p):
        return out_copy(out_slot(over_x, p), over_x, p, 5, to_core)

    def out_relay_xy(p):
        return out_copy(out_slot(over_xy, p), over_xy, p, 6, to_core)

    for p in range(tiles):
        fin[p * tile : (p + 1) * tile, :] = (
            shaped[p * tile : (p + 1) * tile, :] * graft
        ).astype(bf16)
        for copy in out_first(p):
            copy.start()
        out_local(p).start()
    for p in range(tiles):
        out_wait(over_y, p)
        for copy in out_relay_y(p):
            copy.start()
    for p in range(tiles):
        out_wait(over_x, p)
        out_relay_x(p).start()
    for p in range(tiles):
        out_wait(over_xy, p)
        out_relay_xy(p).start()
    for p in range(tiles):
        for xx, yy in ((x, y), (x, 1 - y), (1 - x, y), (1 - x, 1 - y)):
            out_wait((xx, 1 - c, yy), p)
        out_local(p).wait()
        for copy in out_first(p) + out_relay_y(p) + [out_relay_x(p), out_relay_xy(p)]:
            copy.wait_send()

    for copy in o_own_copies + o_relays:
        copy.wait_send()
    for q in range(parts):
        for step, inside in ((1, z < last), (-1, z > 0)):
            @pl.when(inside)
            def _():
                spread(q, step, True).wait_send()

        @pl.when(jnp.logical_not(is_home))
        def _():
            home_remote(q).wait_send()

        for cc in range(2):
            @pl.when(z != zt)
            def _():
                tr_cross(cc, q).wait_send()

            @pl.when(goes_t)
            def _():
                tr_forward(cc, q).wait_send()

            @pl.when(goes_f)
            def _():
                af_forward(cc, q).wait_send()


def routed(planes, activations, out_grads, left_roots, right_roots):
    block = left_roots.shape[1]
    tokens = activations.shape[0]
    parts = 4
    width = block // parts
    dma = pltpu.SemaphoreType.DMA
    return pl.pallas_call(
        functools.partial(kernel, planes, parts),
        out_shape=jax.ShapeDtypeStruct((planes * 2 * block, block // 2), bf16),
        in_specs=[pl.BlockSpec(memory_space=pl.ANY)] * 4,
        out_specs=pl.BlockSpec(memory_space=pl.ANY),
        scratch_shapes=[
            pltpu.VMEM((4, parts, tokens, width), bf16),
            pltpu.VMEM((2, parts, tokens, width), bf16),
            pltpu.VMEM((4, tokens, block), bf16),
            pltpu.VMEM((block, block), f32),
            pltpu.VMEM((block, block), f32),
            pltpu.VMEM((block, block), bf16),
            pltpu.VMEM((block, block), bf16),
            pltpu.VMEM((block, block), bf16),
            pltpu.VMEM((block, block), bf16),
            pltpu.VMEM((width, block), f32),
            pltpu.VMEM((block, block), f32),
            pltpu.VMEM((block, block), f32),
            pltpu.VMEM((block, block), bf16),
            pltpu.VMEM((1, block), f32),
            pltpu.VMEM((1, block), f32),
            dma((2,)), dma((parts,)), dma((3, parts)), dma((2, parts)), dma((2, parts)),
            dma((2, parts)), dma((4, parts)), dma((2, parts)),
            dma, dma((7,)), dma((8,)), dma((parts,)), dma((7, parts)), dma((8, parts)),
        ],
        compiler_params=pltpu.CompilerParams(
            has_side_effects=True, vmem_limit_bytes=62 * 1024 * 1024
        ),
    )(activations, out_grads, left_roots, right_roots)


def partner(block, axis, distance):
    count = lax.axis_size(axis)
    route = []
    for low in range(count):
        high = low | 1 << distance
        if high != low and high < count:
            route += [(low, high), (high, low)]
    return lax.ppermute(block, axis, route)


def local(activations, out_grads, left_roots, right_roots):
    block_size = left_roots.shape[1]
    half_width = block_size // 2
    parity = lax.axis_index("gy") % 2
    is_even = parity == 0
    gathered = lax.all_gather(activations, "gy", axis=1, tiled=True)
    summed = lax.psum_scatter(
        lax.dot_general(
            gathered, out_grads, (((0,), (0,)), ((), ())), preferred_element_type=jnp.float32
        ),
        "gx",
        scatter_dimension=0,
        tiled=True,
    )
    own_part = lax.dynamic_slice_in_dim(summed, parity * block_size, block_size, 0)
    far_part = lax.dynamic_slice_in_dim(summed, (1 - parity) * block_size, block_size, 0)
    received = partner(far_part, "gy", 0)
    left_block = jnp.where(is_even, own_part, received)
    right_block = jnp.where(is_even, received, own_part)
    grad_block = jnp.concatenate([left_block, right_block], axis=1)
    shaped = jnp.dot(
        jnp.dot(left_roots[0], grad_block, precision=lax.Precision.HIGHEST),
        right_roots[0],
        precision=lax.Precision.HIGHEST,
    )
    graft = jnp.sqrt(jnp.mean(grad_block * grad_block) + epsilon) / jnp.sqrt(
        jnp.mean(shaped * shaped) + epsilon
    )
    finished = (shaped * graft).astype(jnp.bfloat16)
    own_part = lax.dynamic_slice_in_dim(finished, parity * half_width, half_width, 1)
    far_part = lax.dynamic_slice_in_dim(finished, (1 - parity) * half_width, half_width, 1)
    received = partner(far_part, "gy", 0)
    upper_rows = jnp.where(is_even, own_part, received)
    lower_rows = jnp.where(is_even, received, own_part)
    paired = jnp.concatenate([upper_rows, lower_rows], axis=0)
    return lax.all_gather(paired, "gx", axis=0, tiled=True)


def solution(mesh):
    in_specs = (
        P("gx", "gy"),
        P("gx", "gy"),
        P(("gx", "gy"), None, None),
        P(("gx", "gy"), None, None),
    )
    out_specs = P(None, "gy")
    n_gx, n_gy = mesh.shape["gx"], mesh.shape["gy"]

    def per_device(activations, out_grads, left_roots, right_roots):
        operands = activations, out_grads, left_roots, right_roots
        block = left_roots.shape[1]
        whole_blocks = activations.shape[1] == block and out_grads.shape[1] * 2 == block
        if n_gx == 4 and n_gy == 2 * n_gx and whole_blocks:
            return routed(n_gx, *operands)
        return local(*operands)

    return jax.shard_map(per_device, mesh=mesh, in_specs=in_specs, out_specs=out_specs, check_vma=False)
```

```python
import functools

import jax
import jax.numpy as jnp
from jax import lax
from jax.experimental import pallas as pl
from jax.experimental.pallas import tpu as pltpu
from jax.sharding import PartitionSpec as P

epsilon = 1e-06
MESH = pl.DeviceIdType.MESH
f32, bf16 = jnp.float32, jnp.bfloat16
COLUMN, ROW = (((0,), (0,)), ((), ())), (((1,), (0,)), ((), ()))


def dot(a, b, dims=ROW):
    return lax.dot_general(a, b, dims, preferred_element_type=f32)


def split(v):
    high = v.astype(bf16)
    return high, (v - high.astype(f32)).astype(bf16)


def kernel(
    planes, parts, a, o, left, right, out,
    af, tr, oall, stage_l, stage_r, lh, ll, rh, rl, grad, half, shaped, fin, sq_g, sq_s,
    load_sem, own_sem, src_sem, fwd_sem, tr_sem, cross_sem, af_recv, tr_recv,
    o_own, o_send, o_recv, out_own, out_send, out_recv,
):
    i, j = lax.axis_index("gx"), lax.axis_index("gy")
    x, c, z, y = i // 2, i % 2, j // 2, j % 2
    block = left.shape[1]
    width = block // parts
    half_width = block // 2
    last = planes - 1

    def dev(xx, cc, zz, yy):
        return (2 * xx + cc, 2 * zz + yy)

    def remote(src, dst, send, recv, to):
        return pltpu.make_async_remote_copy(
            src_ref=src, dst_ref=dst, send_sem=send, recv_sem=recv, device_id=to, device_id_type=MESH
        )

    loads = [
        pltpu.make_async_copy(left.at[0], stage_l, load_sem.at[0]),
        pltpu.make_async_copy(right.at[0], stage_r, load_sem.at[1]),
    ]

    def o_slot(xx, cc, yy):
        columns = pl.ds(pl.multiple_of(yy * half_width, half_width), half_width)
        return oall.at[2 * xx + cc, :, columns]

    def o_copy(src, slot, number, to):
        xx, cc, yy = slot
        return remote(src, o_slot(*slot), o_send.at[number], o_recv.at[4 * xx + 2 * cc + yy], to)

    own, over_x, over_y, over_xy = (x, c, y), (1 - x, c, y), (x, c, 1 - y), (1 - x, c, 1 - y)
    to_x, to_y, to_core = dev(1 - x, c, z, y), dev(x, c, z, 1 - y), dev(x, 1 - c, z, y)
    o_local = pltpu.make_async_copy(o, o_slot(*own), o_own)
    o_own_copies = [o_copy(o, own, 0, to_x), o_copy(o, own, 1, to_y), o_copy(o, own, 2, to_core)]
    o_relays = [
        o_copy(o_slot(*over_x), over_x, 3, to_y),
        o_copy(o_slot(*over_x), over_x, 4, to_core),
        o_copy(o_slot(*over_y), over_y, 5, to_core),
        o_copy(o_slot(*over_xy), over_xy, 6, to_core),
    ]

    def o_wait(slot):
        o_copy(o_slot(*slot), slot, 0, to_x).wait_recv()

    for copy in o_own_copies:
        copy.start()
    o_local.start()

    fx, fc = z // 2, z % 2
    is_home = jnp.logical_and(x == fx, c == fc)
    keeps = x == fx

    def source(q):
        return a.at[:, q * width : (q + 1) * width]

    def home_local(q):
        return pltpu.make_async_copy(source(q), af.at[i, q], own_sem.at[q])

    def home_remote(q):
        return remote(source(q), af.at[i, q], src_sem.at[0, q], af_recv.at[i, q], dev(fx, fc, z, y))

    def spread(q, step, kept):
        number = 1 if step > 0 else 2
        to = dev(x, fc, z + step, y)
        if kept:
            return remote(source(q), af.at[i, q], src_sem.at[number, q], af_recv.at[i, q], to)
        return remote(source(q), tr.at[c, q], src_sem.at[number, q], tr_recv.at[c, q], to)

    for q in range(parts):
        for step, inside in ((1, z < last), (-1, z > 0)):

            @pl.when(jnp.logical_and(inside, keeps))
            def _():
                spread(q, step, True).start()

            @pl.when(jnp.logical_and(inside, jnp.logical_not(keeps)))
            def _():
                spread(q, step, False).start()

        @pl.when(is_home)
        def _():
            home_local(q).start()

    for load in loads:
        load.start()

    zf, zt = i, 2 * (1 - x) + c
    end = jnp.logical_or(z == 0, z == last)
    mid = jnp.logical_not(end)

    def away(origin):
        step = jnp.where(z > origin, 1, -1)
        goes = jnp.logical_and(z != origin, mid)
        return step, goes

    step_f, goes_f = away(zf)
    step_t, goes_t = away(zt)

    def af_forward(cc, q):
        slot = 2 * x + cc
        return remote(
            af.at[slot, q], af.at[slot, q], fwd_sem.at[cc, q], af_recv.at[slot, q],
            dev(x, c, z + step_f, y),
        )

    def tr_forward(cc, q):
        return remote(
            tr.at[cc, q], tr.at[cc, q], tr_sem.at[cc, q], tr_recv.at[cc, q],
            dev(x, c, z + step_t, y),
        )

    def tr_cross(cc, q):
        slot = 2 * x + cc
        return remote(
            tr.at[cc, q], af.at[slot, q], cross_sem.at[cc, q], af_recv.at[slot, q],
            dev(1 - x, c, z, y),
        )

    def af_wait(slot, q):
        remote(
            af.at[slot, q], af.at[slot, q], fwd_sem.at[0, q], af_recv.at[slot, q], to_x
        ).wait_recv()

    def pass_tr(q):
        for cc in range(2):
            @pl.when(z != zt)
            def _():
                remote(
                    tr.at[cc, q], tr.at[cc, q], tr_sem.at[cc, q], tr_recv.at[cc, q], to_x
                ).wait_recv()
                tr_cross(cc, q).start()

            @pl.when(goes_t)
            def _():
                tr_forward(cc, q).start()

    def pass_af(q):
        for cc in range(2):
            @pl.when(goes_f)
            def _():
                af_wait(2 * x + cc, q)
                af_forward(cc, q).start()

    o_wait(over_x)
    o_relays[0].start()
    o_relays[1].start()

    @pl.when(jnp.logical_not(is_home))
    def _():
        for q in range(parts):
            home_remote(q).start()

    @pl.when(mid)
    def _():
        for q in range(parts // 2):
            pass_tr(q)
            pass_af(q)

    o_wait(over_y)
    o_relays[2].start()
    o_wait(over_xy)
    o_relays[3].start()

    early = jnp.logical_and(end, jnp.abs(z - zt) > jnp.abs(z - zf))

    @pl.when(mid)
    def _():
        for q in range(parts // 2, parts):
            pass_tr(q)
            pass_af(q)

    @pl.when(jnp.logical_and(end, jnp.logical_not(early)))
    def _():
        for q in range(parts):
            pass_tr(q)

    for load in loads:
        load.wait()

    tile = 2 * width
    tiles = block // tile

    @pl.loop(0, tiles)
    def _(k):
        rows = pl.ds(pl.multiple_of(k * tile, tile), tile)
        high, low = split(stage_l[rows, :])
        lh[rows, :], ll[rows, :] = high, low
        high, low = split(stage_r[rows, :])
        rh[rows, :], rl[rows, :] = high, low
        half[rows, :] = jnp.zeros((tile, block), f32)

    sq_g[...] = jnp.zeros_like(sq_g)
    sq_s[...] = jnp.zeros_like(sq_s)

    for xx, cc, yy in ((x, 1 - c, y), (1 - x, 1 - c, y), (x, 1 - c, 1 - y), (1 - x, 1 - c, 1 - y)):
        o_wait((xx, cc, yy))
    o_local.wait()

    def wait_part(q):
        for slot in range(4):
            at_home = z == zf

            @pl.when(jnp.logical_and(at_home, slot == i))
            def _():
                home_local(q).wait()

            crossed = jnp.logical_or(slot // 2 != x, end)

            @pl.when(jnp.logical_or(
                jnp.logical_and(at_home, slot != i),
                jnp.logical_and(jnp.logical_not(at_home), crossed),
            ))
            def _():
                af_wait(slot, q)

    for q in range(parts):
        @pl.when(early)
        def _():
            pass_tr(q)

        wait_part(q)
        grad[...] = dot(af[0, q], oall[0], COLUMN)

        @pl.loop(1, 4)
        def _(k):
            grad[...] += dot(af[k, q], oall[k], COLUMN)

        sq_g[...] += jnp.sum(grad[...] * grad[...], axis=0, keepdims=True)
        columns = slice(q * width, (q + 1) * width)

        @pl.loop(0, tiles)
        def _(k):
            rows = pl.ds(pl.multiple_of(k * tile, tile), tile)
            gh, gl = split(grad[...])
            lhk, llk = lh[rows, columns], ll[rows, columns]
            half[rows, :] += dot(lhk, gh) + dot(llk, gh) + dot(lhk, gl)

    @pl.loop(0, tiles)
    def _(k):
        rows = pl.ds(pl.multiple_of(k * tile, tile), tile)
        th, tl = split(half[rows, :])
        value = dot(th, rh[...]) + dot(tl, rh[...]) + dot(th, rl[...])
        shaped[rows, :] = value
        sq_s[...] += jnp.sum(value * value, axis=0, keepdims=True)

    count = block * block
    mean_g = jnp.sum(sq_g[...], axis=1, keepdims=True) / count
    mean_s = jnp.sum(sq_s[...], axis=1, keepdims=True) / count
    graft = jnp.sqrt(mean_g + epsilon) / jnp.sqrt(mean_s + epsilon)

    def out_slot(slot, p):
        xx, cc, yy = slot
        start = (4 * xx + 2 * cc + yy) * block + p * tile
        return out.at[pl.ds(pl.multiple_of(start, tile), tile), :]

    def out_copy(src, slot, p, number, to):
        xx, cc, yy = slot
        return remote(
            src, out_slot(slot, p), out_send.at[number, p], out_recv.at[4 * xx + 2 * cc + yy, p], to
        )

    def out_wait(slot, p):
        out_copy(out_slot(slot, p), slot, p, 0, to_x).wait_recv()

    def fin_part(side, p):
        columns = pl.ds(pl.multiple_of(side * half_width, half_width), half_width)
        return fin.at[p * tile : (p + 1) * tile, columns]

    def out_local(p):
        return pltpu.make_async_copy(fin_part(y, p), out_slot(own, p), out_own.at[p])

    def out_first(p):
        return [
            out_copy(fin_part(1 - y, p), own, p, 0, to_y),
            out_copy(fin_part(y, p), own, p, 1, to_x),
            out_copy(fin_part(y, p), own, p, 2, to_core),
        ]

    def out_relay_y(p):
        return [
            out_copy(out_slot(over_y, p), over_y, p, 3, to_x),
            out_copy(out_slot(over_y, p), over_y, p, 4, to_core),
        ]

    def out_relay_x(p):
        return out_copy(out_slot(over_x, p), over_x, p, 5, to_core)

    def out_relay_xy(p):
        return out_copy(out_slot(over_xy, p), over_xy, p, 6, to_core)

    for p in range(tiles):
        fin[p * tile : (p + 1) * tile, :] = (
            shaped[p * tile : (p + 1) * tile, :] * graft
        ).astype(bf16)
        for copy in out_first(p):
            copy.start()
        out_local(p).start()
    for p in range(tiles):
        out_wait(over_y, p)
        for copy in out_relay_y(p):
            copy.start()
    for p in range(tiles):
        out_wait(over_x, p)
        out_relay_x(p).start()
    for p in range(tiles):
        out_wait(over_xy, p)
        out_relay_xy(p).start()
    for p in range(tiles):
        for xx, yy in ((x, y), (x, 1 - y), (1 - x, y), (1 - x, 1 - y)):
            out_wait((xx, 1 - c, yy), p)
        out_local(p).wait()
        for copy in out_first(p) + out_relay_y(p) + [out_relay_x(p), out_relay_xy(p)]:
            copy.wait_send()

    for copy in o_own_copies + o_relays:
        copy.wait_send()
    for q in range(parts):
        for step, inside in ((1, z < last), (-1, z > 0)):
            @pl.when(inside)
            def _():
                spread(q, step, True).wait_send()

        @pl.when(jnp.logical_not(is_home))
        def _():
            home_remote(q).wait_send()

        for cc in range(2):
            @pl.when(z != zt)
            def _():
                tr_cross(cc, q).wait_send()

            @pl.when(goes_t)
            def _():
                tr_forward(cc, q).wait_send()

            @pl.when(goes_f)
            def _():
                af_forward(cc, q).wait_send()


def routed(planes, activations, out_grads, left_roots, right_roots):
    block = left_roots.shape[1]
    tokens = activations.shape[0]
    parts = 8
    width = block // parts
    dma = pltpu.SemaphoreType.DMA
    return pl.pallas_call(
        functools.partial(kernel, planes, parts),
        out_shape=jax.ShapeDtypeStruct((planes * 2 * block, block // 2), bf16),
        in_specs=[pl.BlockSpec(memory_space=pl.ANY)] * 4,
        out_specs=pl.BlockSpec(memory_space=pl.ANY),
        scratch_shapes=[
            pltpu.VMEM((4, parts, tokens, width), bf16),
            pltpu.VMEM((2, parts, tokens, width), bf16),
            pltpu.VMEM((4, tokens, block), bf16),
            pltpu.VMEM((block, block), f32),
            pltpu.VMEM((block, block), f32),
            pltpu.VMEM((block, block), bf16),
            pltpu.VMEM((block, block), bf16),
            pltpu.VMEM((block, block), bf16),
            pltpu.VMEM((block, block), bf16),
            pltpu.VMEM((width, block), f32),
            pltpu.VMEM((block, block), f32),
            pltpu.VMEM((block, block), f32),
            pltpu.VMEM((block, block), bf16),
            pltpu.VMEM((1, block), f32),
            pltpu.VMEM((1, block), f32),
            dma((2,)), dma((parts,)), dma((3, parts)), dma((2, parts)), dma((2, parts)),
            dma((2, parts)), dma((4, parts)), dma((2, parts)),
            dma, dma((7,)), dma((8,)), dma((parts,)), dma((7, parts)), dma((8, parts)),
        ],
        compiler_params=pltpu.CompilerParams(
            has_side_effects=True, vmem_limit_bytes=62 * 1024 * 1024
        ),
    )(activations, out_grads, left_roots, right_roots)


def partner(block, axis, distance):
    count = lax.axis_size(axis)
    route = []
    for low in range(count):
        high = low | 1 << distance
        if high != low and high < count:
            route += [(low, high), (high, low)]
    return lax.ppermute(block, axis, route)


def local(activations, out_grads, left_roots, right_roots):
    block_size = left_roots.shape[1]
    half_width = block_size // 2
    parity = lax.axis_index("gy") % 2
    is_even = parity == 0
    gathered = lax.all_gather(activations, "gy", axis=1, tiled=True)
    summed = lax.psum_scatter(
        lax.dot_general(
            gathered, out_grads, (((0,), (0,)), ((), ())), preferred_element_type=jnp.float32
        ),
        "gx",
        scatter_dimension=0,
        tiled=True,
    )
    own_part = lax.dynamic_slice_in_dim(summed, parity * block_size, block_size, 0)
    far_part = lax.dynamic_slice_in_dim(summed, (1 - parity) * block_size, block_size, 0)
    received = partner(far_part, "gy", 0)
    left_block = jnp.where(is_even, own_part, received)
    right_block = jnp.where(is_even, received, own_part)
    grad_block = jnp.concatenate([left_block, right_block], axis=1)
    shaped = jnp.dot(
        jnp.dot(left_roots[0], grad_block, precision=lax.Precision.HIGHEST),
        right_roots[0],
        precision=lax.Precision.HIGHEST,
    )
    graft = jnp.sqrt(jnp.mean(grad_block * grad_block) + epsilon) / jnp.sqrt(
        jnp.mean(shaped * shaped) + epsilon
    )
    finished = (shaped * graft).astype(jnp.bfloat16)
    own_part = lax.dynamic_slice_in_dim(finished, parity * half_width, half_width, 1)
    far_part = lax.dynamic_slice_in_dim(finished, (1 - parity) * half_width, half_width, 1)
    received = partner(far_part, "gy", 0)
    upper_rows = jnp.where(is_even, own_part, received)
    lower_rows = jnp.where(is_even, received, own_part)
    paired = jnp.concatenate([upper_rows, lower_rows], axis=0)
    return lax.all_gather(paired, "gx", axis=0, tiled=True)


def solution(mesh):
    in_specs = (
        P("gx", "gy"),
        P("gx", "gy"),
        P(("gx", "gy"), None, None),
        P(("gx", "gy"), None, None),
    )
    out_specs = P(None, "gy")
    n_gx, n_gy = mesh.shape["gx"], mesh.shape["gy"]

    def per_device(activations, out_grads, left_roots, right_roots):
        operands = activations, out_grads, left_roots, right_roots
        block = left_roots.shape[1]
        whole_blocks = activations.shape[1] == block and out_grads.shape[1] * 2 == block
        if n_gx == 4 and n_gy == 2 * n_gx and whole_blocks:
            return routed(n_gx, *operands)
        return local(*operands)

    return jax.shard_map(per_device, mesh=mesh, in_specs=in_specs, out_specs=out_specs, check_vma=False)
```
